32 devices in a mesh: row: 16 (over z, x, core), col: 2 (over y).
Axes of the slice: x: 2, y: 2, z: 4, core: 2. Of those that a mesh axis runs over, the one named last changes fastest.
Arguments:
- particles: bfloat16 [64, 64, 4096], P(('row', 'col')), may hold values from -6 to 6
- orientation: int32 [64], P(('row', 'col')), may hold values from 0 to 23
- tilt: int32 [64], P(('row', 'col')), may hold values from 0 to 7
- weight: float32 [64], P(('row', 'col')), may hold values from 0.3 to 3
Outputs:
- reference_map: float32 [2, 64, 4096], P(None, 'row', 'col')
The draws below stay inside these ranges and needn't reach their ends.
Inputs may be any that keep to these rules, and one draw needn't show every extreme that they name: `orientation`: an index into the table of 24 rotations. `tilt`: an index into the 8 tilt ranges.
All inputs are finite; a program needn't handle non-finite values.
Results may differ from the reference program's by a relative error of at most 0.0054.
Values sent between devices are 32-bit elements; how exact they have to be, the bound alone decides.
A program may use at most 64 MiB of HBM per device.

```python
import math
from functools import partial
import jax
import jax.numpy as jnp
from jax import lax

L = 64
ROTATIONS = 24
TILTS = 8
PARTICLES = 64
N_ROW = 16
N_COL = 2


def plant(drawn, rng, smallest, top_value):
    index_at = [jax.random.randint(jax.random.fold_in(rng, axis), (), 0, length) for axis, length in enumerate(drawn.shape)]
    main_axis = drawn.shape.index(max(drawn.shape))
    next_to = index_at[:main_axis] + [(index_at[main_axis] + 1) % drawn.shape[main_axis]] + index_at[main_axis + 1:]
    return drawn.at[tuple(index_at)].set(smallest).at[tuple(next_to)].set(top_value)


def block_levels(key, shape, pieces, smallest, top_value):
    gain, own = 1.0, jax.random.fold_in(key, 6)
    for dim, parts in pieces:
        draws = jnp.exp(jax.random.uniform(jax.random.fold_in(own, dim), (parts,), jnp.float32, smallest / len(pieces), top_value / len(pieces)))
        gain = gain * jnp.repeat(draws, shape[dim] // parts).reshape([-1 if axis == dim else 1 for axis in range(len(shape))])
    return gain


def noise(rng, shape, scale, reach, shards=(), held_as=jnp.bfloat16):
    loudness = block_levels(rng, shape, shards, -0.22, 0.18) if shards else 1.0
    values = jax.random.normal(rng, shape, jnp.float32) * scale * loudness
    return jnp.minimum(jnp.maximum(values, -reach), reach).astype(held_as)


def setup_inputs(seed: int = 0) -> dict:
    seeds = jax.random.split(jax.random.key(seed), 5)
    return {
        "particles": noise(seeds[0], (PARTICLES, L, L * L), 1.0, 6.0, ((0, 32),)),
        "orientation": plant(jax.random.randint(seeds[1], (PARTICLES,), 0, ROTATIONS), jax.random.fold_in(seeds[1], 1), 0, ROTATIONS - 1).astype(jnp.int32),
        "tilt": plant(jax.random.randint(seeds[2], (PARTICLES,), 0, TILTS), jax.random.fold_in(seeds[2], 1), 0, TILTS - 1).astype(jnp.int32),
        "weight": jnp.clip(jnp.exp(math.log(3.0) - 2.3025851 * jax.random.uniform(seeds[3], (PARTICLES,), jnp.float32) ** block_levels(seeds[3], (PARTICLES,), ((0, 32),), -0.2, 0.2)), 0.3, 3.0),
    }


PERM_LIST = ((0, 1, 2), (0, 2, 1), (1, 0, 2), (1, 2, 0), (2, 0, 1), (2, 1, 0))
PARITY_LIST = (0, 1, 1, 0, 0, 1)
BEAM_LIST = (0, 0, 1, 2, 1, 2)
ACROSS_LIST = (2, 1, 2, 1, 0, 0)
wiener_offset = 1.0

def dft_tables(width):
    index = jnp.arange(width, dtype=jnp.int32)
    phase = index[:, None] * index[None, :] % width
    angle = phase.astype(jnp.float32) * (2.0 * math.pi / width)
    factor = 1.0 / math.sqrt(width)
    return ((jnp.cos(angle) * factor).astype(jnp.bfloat16), (jnp.sin(angle) * factor).astype(jnp.bfloat16))

def rotate(volume, orient):
    perm_index = orient // 4
    flip_first = orient % 2
    flip_second = orient // 2 % 2
    parity = jnp.array(PARITY_LIST, jnp.int32)[perm_index]
    flip_third = (flip_first + flip_second + parity) % 2
    volume = jnp.where(flip_first == 1, jnp.flip(volume, 0), volume)
    volume = jnp.where(flip_second == 1, jnp.flip(volume, 1), volume)
    volume = jnp.where(flip_third == 1, jnp.flip(volume, 2), volume)
    branches = [partial(jnp.transpose, axes=ordering) for ordering in PERM_LIST]
    return lax.switch(perm_index, branches, volume)

def plane_transform(volume, orient, cosines, sines):
    width = cosines.shape[0]
    cube = rotate(volume.reshape(width, width, width), orient)
    flat = cube.reshape(width * width, width)
    real_part = jnp.dot(flat, cosines, preferred_element_type=jnp.float32)
    imag_part = -jnp.dot(flat, sines, preferred_element_type=jnp.float32)
    first = jnp.stack([real_part, imag_part]).astype(jnp.bfloat16).reshape(2, width, width, width)
    first_wide = first.astype(jnp.float32)
    cos_part = jnp.einsum('ky,pzyx->pzkx', cosines.astype(jnp.float32), first_wide)
    sin_part = jnp.einsum('ky,pzyx->pzkx', sines.astype(jnp.float32), first_wide)
    spec_real = cos_part[0] + sin_part[1]
    spec_imag = cos_part[1] - sin_part[0]
    return jnp.stack([spec_real, spec_imag]).astype(jnp.bfloat16).reshape(2, width, width * width)

def frequency(index, width):
    return jnp.abs(jnp.where(index < width // 2, index, index - width))

def wedge_mask(orient, tilt_index, row_start, row_count, width):
    perm_index = orient // 4
    beam = jnp.array(BEAM_LIST, jnp.int32)[perm_index]
    across = jnp.array(ACROSS_LIST, jnp.int32)[perm_index]
    first_axis = frequency(row_start + jnp.arange(row_count, dtype=jnp.int32), width)[:, None, None]
    middle = frequency(jnp.arange(width, dtype=jnp.int32), width)[None, :, None]
    last_axis = frequency(jnp.arange(width, dtype=jnp.int32), width)[None, None, :]
    along_beam = jnp.where(beam == 0, first_axis, jnp.where(beam == 1, middle, last_axis))
    along_across = jnp.where(across == 0, first_axis, jnp.where(across == 1, middle, last_axis))
    inside = 4 * along_beam <= (5 + 2 * tilt_index) * along_across
    return inside.astype(jnp.float32).reshape(row_count, width * width)

def slab_terms(spectra, orientation, tilt, weight, cosines, sines, row_start, row_count):
    width = cosines.shape[0]
    rows_cos = lax.dynamic_slice_in_dim(cosines, row_start, row_count, 0)
    rows_sin = lax.dynamic_slice_in_dim(sines, row_start, row_count, 0)
    rows_both = jnp.concatenate([rows_cos, rows_sin], axis=0)

    def add_one(totals, item):
        spectrum, orient, tilt_index, scale = item
        from_real = jnp.dot(rows_both, spectrum[0], preferred_element_type=jnp.float32)
        from_imag = jnp.dot(rows_both, spectrum[1], preferred_element_type=jnp.float32)
        real_part = from_real[:row_count] + from_imag[row_count:]
        imag_part = from_imag[:row_count] - from_real[row_count:]
        weighted = scale * wedge_mask(orient, tilt_index, row_start, row_count, width)
        return ((totals[0] + weighted * real_part, totals[1] + weighted * imag_part, totals[2] + weighted), None)
    zeros = jnp.zeros((row_count, width * width), jnp.float32)
    totals, _ = lax.scan(add_one, (zeros, zeros, zeros), (spectra, orientation, tilt, weight))
    return jnp.stack(totals, axis=1)

def finish(owned):
    result = owned[:, 0:2] / jnp.sqrt(owned[:, 2:3] + wiener_offset)
    return jnp.transpose(result, (1, 0, 2))

def reference(particles, orientation, tilt, weight):
    width = particles.shape[1]
    cosines, sines = dft_tables(width)
    blocks = N_ROW * N_COL
    per_block = particles.shape[0] // blocks

    def one_block(carry, item):
        volumes, orients, tilts, scales = item
        spectra = jax.vmap(plane_transform, in_axes=(0, 0, None, None))(volumes, orients, cosines, sines)
        return (carry + slab_terms(spectra, orients, tilts, scales, cosines, sines, 0, width), None)
    start_sum = jnp.zeros((width, 3, width * width), jnp.float32)
    items = (particles.reshape(blocks, per_block, width, width * width), orientation.reshape(blocks, per_block), tilt.reshape(blocks, per_block), weight.reshape(blocks, per_block))
    total, _ = lax.scan(one_block, start_sum, items)
    return finish(total)
```

```python
import math

import jax
import jax.numpy as jnp
import numpy as np
from jax import lax
from jax.experimental import pallas as pl
from jax.experimental.pallas import tpu as pltpu
from jax.sharding import PartitionSpec as P

TILTS = 8
BEAM_LIST = (0, 0, 1, 2, 1, 2)
ACROSS_LIST = (2, 1, 2, 1, 0, 0)
wiener_offset = 1.0
MESH = pl.DeviceIdType.MESH
PAD = 8
UNROLL = 32


def tables(width):
    index = np.arange(width)
    angle = (index[:, None] * index[None, :] % width).astype(np.float32) * np.float32(2.0 * math.pi / width)
    factor = np.float32(1.0 / math.sqrt(width))
    pairs, planes, rows, cols = [], [], [], []
    for reverse in (False, True):
        c, s = np.cos(angle) * factor, np.sin(angle) * factor
        if reverse:
            c, s = c[:, ::-1], s[:, ::-1]
        plain = np.concatenate([c.T, -s.T], 1)
        turned = np.concatenate([-s.T, -c.T], 1)
        zero = np.zeros_like(plain)
        pairs.append(np.block([[plain, zero, turned, zero], [zero, plain, zero, turned]]))
        planes.append(np.concatenate([plain, turned], 1))
        rows.append(np.concatenate([c, s], 1))
        cols.append(np.concatenate([c, s], 1).T)
    return [jnp.asarray(np.stack(t), jnp.float32).astype(jnp.bfloat16) for t in (pairs, planes, rows, cols)]


def frequency(index, width):
    return jnp.abs(jnp.where(index < width // 2, index, index - width))


def transform_kernel(width, ori, tilt, weight, x_ref, pair_ref, plane_ref, row_ref, col_ref, acc_ref, cls_ref, held):
    p = pl.program_id(0)
    wide = 2 * width
    step = width + PAD
    orient = ori[p]
    perm = orient // 4
    flip_z = orient % 2
    flip_y = orient // 2 % 2
    parity = jnp.where((perm == 1) | (perm == 2) | (perm == 5), 1, 0)
    flip_x = (flip_z + flip_y + parity) % 2
    swapped = perm >= 3
    scale = weight[p]

    @pl.when(p == 0)
    def _():
        acc_ref[...] = jnp.zeros_like(acc_ref)
        cls_ref[...] = jnp.zeros_like(cls_ref)

    label = lax.broadcasted_iota(jnp.int32, cls_ref.shape, 1)
    cls_ref[...] += jnp.where(label == perm * TILTS + tilt[p], scale, 0.0)

    down = frequency(lax.broadcasted_iota(jnp.int32, (width, wide), 0), width)
    along = frequency(lax.broadcasted_iota(jnp.int32, (width, wide), 1) % width, width)
    beam = jnp.where(swapped, along, down)
    across = jnp.where(swapped, down, along)
    mask = jnp.where(4 * beam <= (5 + 2 * tilt[p]) * across, scale, 0.0)

    def planes_of(turn, table):
        rows = row_ref[table]

        def steps(i, carry):
            start = pl.multiple_of(i * (UNROLL * wide), UNROLL * wide)
            for u, rhs in enumerate(turn(x_ref[0, :, pl.ds(start, UNROLL * wide)])):
                j = i * UNROLL + u
                out = jnp.dot(rows, rhs, preferred_element_type=jnp.float32)
                held[pl.ds(2 * j, width, stride=step), :] = out[:, :wide] * mask
                held[pl.ds(2 * j + 1, width, stride=step), :] = out[:, wide:] * mask
            return carry

        lax.fori_loop(0, width // 2 // UNROLL, steps, 0)

    @pl.when(jnp.logical_not(swapped))
    def _():
        table = pair_ref[flip_x]

        def turn(block):
            tall = jnp.concatenate([block[:, u * wide : (u + 1) * wide] for u in range(UNROLL)], 0)
            out = jnp.dot(tall, table, preferred_element_type=jnp.float32)
            for u in range(UNROLL):
                part = out[u * width : (u + 1) * width]
                yield jnp.concatenate([part[:, : 2 * wide], part[:, 2 * wide :]], 0).astype(jnp.bfloat16)

        planes_of(turn, flip_z)

    @pl.when(swapped)
    def _():
        table = plane_ref[flip_z]

        def turn(block):
            out = lax.dot_general(block, table, (((0,), (0,)), ((), ())), preferred_element_type=jnp.float32)
            for u in range(UNROLL):
                a = out[u * wide : u * wide + width]
                b = out[u * wide + width : (u + 1) * wide]
                upper = jnp.concatenate([a[:, :wide], b[:, :wide]], 1)
                lower = jnp.concatenate([a[:, wide:], b[:, wide:]], 1)
                yield jnp.concatenate([upper, lower], 0).astype(jnp.bfloat16)

        planes_of(turn, flip_x)

    sign = jnp.where(lax.broadcasted_iota(jnp.int32, (width, wide), 1) < width, 1.0, -1.0)

    def last_of(put):
        def steps(i, carry):
            stacks = []
            for u in range(UNROLL):
                s = (i * UNROLL + u) * 2
                a = held[pl.ds(pl.multiple_of(s * step, 8), width), :]
                b = held[pl.ds(pl.multiple_of(s * step + step, 8), width), :]
                upper = jnp.concatenate([a, b], 1)
                lower = jnp.concatenate([pltpu.roll(a, width, 1) * sign, pltpu.roll(b, width, 1) * sign], 1)
                stacks.append(jnp.concatenate([upper, lower], 0).astype(jnp.bfloat16))
            put(i * UNROLL * 2, stacks)
            return carry

        lax.fori_loop(0, width // 2 // UNROLL, steps, 0)

    @pl.when((perm == 0) | (perm == 5))
    def _():
        table = row_ref[flip_y]

        def put(s, stacks):
            for u, rhs in enumerate(stacks):
                out = jnp.dot(table, rhs, preferred_element_type=jnp.float32)
                at = pl.multiple_of((s + 2 * u) * step, 8)
                acc_ref[pl.ds(at, width), :] += out[:, :wide]
                acc_ref[pl.ds(pl.multiple_of(at + step, 8), width), :] += out[:, wide:]

        last_of(put)

    @pl.when((perm == 1) | (perm == 4))
    def _():
        table = col_ref[flip_y]

        def put(s, stacks):
            out = lax.dot_general(
                jnp.concatenate(stacks, 1), table, (((0,), (0,)), ((), ())), preferred_element_type=jnp.float32
            )
            for k in range(2 * len(stacks)):
                part = jnp.concatenate([out[k * wide : k * wide + width], out[k * wide + width : (k + 1) * wide]], 1)
                acc_ref[pl.ds(pl.multiple_of((s + k) * step, 8), width), :] += part

        last_of(put)

    @pl.when((perm == 2) | (perm == 3))
    def _():
        table = row_ref[flip_y]

        def put(s, stacks):
            for u, rhs in enumerate(stacks):
                out = jnp.dot(table, rhs, preferred_element_type=jnp.float32)
                acc_ref[pl.ds(s + 2 * u, width, stride=step), :] += out[:, :wide]
                acc_ref[pl.ds(s + 2 * u + 1, width, stride=step), :] += out[:, wide:]

        last_of(put)


def transform(particles, orientation, tilt, weight):
    count, width, area = particles.shape
    step = width + PAD
    consts = tables(width)
    smem = pl.BlockSpec(memory_space=pltpu.SMEM)
    whole = [pl.BlockSpec(t.shape, lambda i: (0, 0, 0)) for t in consts]
    return pl.pallas_call(
        lambda *refs: transform_kernel(width, *refs),
        grid=(count,),
        in_specs=[smem, smem, smem, pl.BlockSpec((1, width, area), lambda i: (i, 0, 0))] + whole,
        out_specs=[
            pl.BlockSpec(memory_space=pltpu.VMEM),
            pl.BlockSpec(memory_space=pltpu.VMEM),
        ],
        out_shape=[
            pltpu.VMEM((width * step, 2 * width), jnp.float32),
            pltpu.VMEM((8, 128), jnp.float32),
        ],
        scratch_shapes=[pltpu.VMEM((width * step, 2 * width), jnp.float32)],
        name="transform",
    )(orientation, tilt, weight, particles, *consts)


def exchange_kernel(
    n_z, n_col, width, acc, cls, fin, got1, sum1, got2, sum2, got3,
    zgot, zsum, ygot, cgot1, csum1, cgot2, csum2, cgot3, s1, r1, s2, r2, s3, r3, cs1, cr1, cs2, cr2, cs3, cr3, sz, rz, sy, ry,
):
    row, col = lax.axis_index("row"), lax.axis_index("col")
    z, x, core = row // 4, row // 2 % 2, row % 2
    band = width // n_col
    group = 2 * n_col
    member = x * n_col + col
    pair = (row + 1 - 2 * core, col)

    def mate(k):
        m = lax.rem(member + k, group)
        return m, (z * 4 + m // n_col * 2 + core, lax.rem(m, n_col))

    def far(k):
        t = lax.rem(z + k, n_z)
        return t, (t * 4 + x * 2 + core, col)

    def send(src, dst, ssem, rsem, to):
        copy = pltpu.make_async_remote_copy(
            src_ref=src, dst_ref=dst, send_sem=ssem, recv_sem=rsem, device_id=to, device_id_type=MESH
        )
        copy.start()
        return copy

    barrier = pltpu.get_barrier_semaphore()
    others = [pair] + [mate(k)[1] for k in range(1, group)] + [far(k)[1] for k in range(1, n_z)]
    for other in others:
        pl.semaphore_signal(barrier, inc=1, device_id=other, device_id_type=MESH)
    pl.semaphore_wait(barrier, len(others))

    def bands(m):
        return pl.ds(pl.multiple_of(lax.rem(m, n_col) * band, 8), band)

    small1 = send(cls, cgot1, cs1, cr1, pair)
    first = []
    for k in range(n_z):
        t = lax.rem(z + 1 + k, n_z)
        first.append(send(acc.at[t, :, 1 - core, :, pl.ds(0, width), :], got1.at[k], s1.at[k], r1.at[k], pair))
    small1.wait()
    csum1[...] = cls[...] + cgot1[...]
    small2 = [send(csum1, cgot2.at[k], cs2.at[k], cr2.at[k], mate(k + 1)[1]) for k in range(group - 1)]
    planes = fin.shape[0]
    main = planes - 1
    second, across_z = [], []
    for k in range(n_z):
        t = lax.rem(z + 1 + k, n_z)
        first[k].wait()
        for half in range(2):
            sum1[k, half] = acc[t, half, core, :, pl.ds(0, width), :] + got1[k, half]
        for g in range(group - 1):
            m, to = mate(g + 1)
            second.append(
                send(
                    sum1.at[k, m // n_col, pl.ds(0, main), bands(m), :], got2.at[k, g], s2.at[k, g], r2.at[k, g], to
                )
            )
        if k < n_z - 1:
            across_z.append(send(sum1.at[k, :, main], zgot.at[k], sz.at[k], rz.at[k], far(k + 1)[1]))
    for copy in small2:
        copy.wait()
    small = csum1[...]
    for k in range(group - 1):
        small = small + cgot2[k]
    csum2[...] = small
    small3 = [send(csum2, cgot3.at[k], cs3.at[k], cr3.at[k], far(k + 1)[1]) for k in range(n_z - 1)]
    third = []
    for k in range(n_z):
        for g in range(group - 1):
            second[k * (group - 1) + g].wait()
        total = sum1[k, x, pl.ds(0, main), bands(member), :]
        for g in range(group - 1):
            total = total + got2[k, g]
        sum2[k] = total
        if k < n_z - 1:
            third.append(send(sum2.at[k], got3.at[k], s3.at[k], r3.at[k], far(k + 1)[1]))
        if k == n_z // 2 - 1:
            for copy in across_z:
                copy.wait()
            for half in range(2):
                total = sum1[n_z - 1, half, main]
                for d in range(n_z - 1):
                    total = total + zgot[d, half]
                zsum[half] = total
            closing = []
            for g in range(group - 1):
                m, to = mate(g + 1)
                closing.append(send(zsum.at[m // n_col, bands(m), :], ygot.at[g], sy.at[g], ry.at[g], to))

    for copy in small3:
        copy.wait()
    small = csum2[...]
    for k in range(n_z - 1):
        small = small + cgot3[k]
    shape = (band, 2 * width)
    middle = frequency(col * band + lax.broadcasted_iota(jnp.int32, shape, 0), width)
    last = frequency(lax.broadcasted_iota(jnp.int32, shape, 1) % width, width)
    factors = []
    for plane in range(planes):
        axes = (jnp.full(shape, 1, jnp.int32) * frequency(row * planes + plane, width), middle, last)
        total = jnp.zeros(shape, jnp.float32)
        for perm in range(6):
            beam, across = 4 * axes[BEAM_LIST[perm]], axes[ACROSS_LIST[perm]]
            for tilt in range(TILTS):
                share = small[0:1, perm * TILTS + tilt : perm * TILTS + tilt + 1]
                total = total + jnp.where(beam <= (5 + 2 * tilt) * across, share, 0.0)
        factors.append(jnp.sqrt(total + wiener_offset))
    for copy in third + closing:
        copy.wait()
    for plane in range(planes):
        if plane < main:
            value = sum2[n_z - 1, plane]
            for k in range(n_z - 1):
                value = value + got3[k, plane]
        else:
            value = zsum[x, bands(member), :]
            for g in range(group - 1):
                value = value + ygot[g]
        fin[plane] = value / factors[plane]


def finish_kernel(width, fin, out):
    planes, band, _ = fin.shape
    half = band // 2
    left = lax.broadcasted_iota(jnp.int32, (half, 2 * width), 1) < width
    for plane in range(planes):
        even = fin[plane, pl.ds(0, half, stride=2), :]
        odd = fin[plane, pl.ds(1, half, stride=2), :]
        real = jnp.where(left, even, pltpu.roll(odd, width, 1))
        imag = jnp.where(left, pltpu.roll(even, width, 1), odd)
        for k in range(half):
            lanes = pl.ds(k * 2 * width, 2 * width)
            out[0, plane : plane + 1, lanes] = real[k : k + 1]
            out[1, plane : plane + 1, lanes] = imag[k : k + 1]


def finish(fin, width):
    planes, band, _ = fin.shape
    vmem = pl.BlockSpec(memory_space=pltpu.VMEM)
    return pl.pallas_call(
        lambda *refs: finish_kernel(width, *refs),
        in_specs=[vmem],
        out_specs=vmem,
        out_shape=jax.ShapeDtypeStruct((2, planes, band * width), jnp.float32),
        name="finish",
    )(pltpu.with_memory_space_constraint(fin, pltpu.VMEM))


def exchange(acc, cls, n_row, n_col, width):
    n_z = n_row // 4
    planes = width // n_row
    band = width // n_col
    group = 2 * n_col
    wide = 2 * width
    acc = acc.reshape(n_z, 2, 2, planes, width + PAD, wide)
    acc = pltpu.with_memory_space_constraint(acc, pltpu.VMEM)
    cls = pltpu.with_memory_space_constraint(cls, pltpu.VMEM)
    vmem = pl.BlockSpec(memory_space=pltpu.VMEM)
    f32 = jnp.float32
    dma = pltpu.SemaphoreType.DMA
    return pl.pallas_call(
        lambda *refs: exchange_kernel(n_z, n_col, width, *refs),
        in_specs=[vmem, vmem],
        out_specs=vmem,
        out_shape=pltpu.VMEM((planes, band, wide), f32),
        scratch_shapes=[
            pltpu.VMEM((n_z, 2, planes, width, wide), f32),
            pltpu.VMEM((n_z, 2, planes, width, wide), f32),
            pltpu.VMEM((n_z, group - 1, planes - 1, band, wide), f32),
            pltpu.VMEM((n_z, planes - 1, band, wide), f32),
            pltpu.VMEM((n_z - 1, planes - 1, band, wide), f32),
            pltpu.VMEM((n_z - 1, 2, width, wide), f32),
            pltpu.VMEM((2, width, wide), f32),
            pltpu.VMEM((group - 1, band, wide), f32),
            pltpu.VMEM((8, 128), f32),
            pltpu.VMEM((8, 128), f32),
            pltpu.VMEM((group - 1, 8, 128), f32),
            pltpu.VMEM((8, 128), f32),
            pltpu.VMEM((n_z - 1, 8, 128), f32),
            dma((n_z,)), dma((n_z,)), dma((n_z, group - 1)), dma((n_z, group - 1)),
            dma((n_z - 1,)), dma((n_z - 1,)),
            dma, dma, dma((group - 1,)), dma((group - 1,)), dma((n_z - 1,)), dma((n_z - 1,)),
            dma((n_z - 1,)), dma((n_z - 1,)), dma((group - 1,)), dma((group - 1,)),
        ],
        compiler_params=pltpu.CompilerParams(collective_id=0, has_side_effects=True),
        name="exchange",
    )(acc, cls)


def solution(mesh):
    n_row, n_col = mesh.shape["row"], mesh.shape["col"]

    def body(particles, orientation, tilt, weight):
        width = particles.shape[1]
        acc, cls = transform(particles, orientation, tilt, weight)
        return finish(exchange(acc, cls, n_row, n_col, width), width)

    placed = (P(("row", "col"), None, None), P(("row", "col")), P(("row", "col")), P(("row", "col")))
    return jax.shard_map(body, mesh=mesh, in_specs=placed, out_specs=P(None, "row", "col"), check_vma=False)
```

```python
import math

import jax
import jax.numpy as jnp
import numpy as np
from jax import lax
from jax.experimental import pallas as pl
from jax.experimental.pallas import tpu as pltpu
from jax.sharding import PartitionSpec as P

TILTS = 8
BEAM_LIST = (0, 0, 1, 2, 1, 2)
ACROSS_LIST = (2, 1, 2, 1, 0, 0)
wiener_offset = 1.0
MESH = pl.DeviceIdType.MESH
PAD = 8
BLOCKS = 8


def tables(width):
    index = np.arange(width)
    angle = (index[:, None] * index[None, :] % width).astype(np.float32) * np.float32(2.0 * math.pi / width)
    factor = np.float32(1.0 / math.sqrt(width))
    lefts, turns, rights, rows = [], [], [], []
    for reverse in (False, True):
        c, s = np.cos(angle) * factor, np.sin(angle) * factor
        if reverse:
            c, s = c[:, ::-1], s[:, ::-1]
        zero = np.zeros_like(c)
        lefts.append(np.concatenate([c, -s], 0))
        turns.append(np.block([[c, zero], [-s, zero], [zero, c], [zero, -s]]))
        plain, turned, blank = np.concatenate([c.T, -s.T], 1), np.concatenate([s.T, c.T], 1), np.zeros((width, 2 * width))
        rights.append(np.block([[plain, blank], [blank, plain], [turned, blank], [blank, turned]]))
        rows.append(np.concatenate([c, s], 1))
    return [jnp.asarray(np.stack(t), jnp.float32).astype(jnp.bfloat16) for t in (lefts, turns, rights, rows)]


def frequency(index, width):
    return jnp.abs(jnp.where(index < width // 2, index, index - width))


def transform_kernel(
    width, ori, tilt, weight, x_ref, left_ref, turn_ref, right_ref, row_ref, held, rows_out, par_ref, cls_ref, loose, cube
):
    p = pl.program_id(0)
    wide = 2 * width
    half = width // 2
    step = width + PAD
    orient = ori[p]
    perm = orient // 4
    flip_z = orient % 2
    flip_y = orient // 2 % 2
    parity = jnp.where((perm == 1) | (perm == 2) | (perm == 5), 1, 0)
    flip_x = (flip_z + flip_y + parity) % 2
    swapped = (perm == 1) | (perm == 4) | (perm == 5)
    whole = (perm == 0) | (perm == 5)
    outer = (perm == 2) | (perm == 4)
    scale = weight[p]

    @pl.when(p == 0)
    def _():
        cls_ref[...] = jnp.zeros_like(cls_ref)

    label = lax.broadcasted_iota(jnp.int32, cls_ref.shape, 1)
    cls_ref[...] += jnp.where(label == perm * TILTS + tilt[p], scale, 0.0)

    slope = (5 + 2 * tilt[p]).astype(jnp.float32)
    line = lax.broadcasted_iota(jnp.int32, (8, wide), 0)
    par = jnp.where(line == 3, scale, 0.0)
    for perm_index in range(6):
        here = (line == BEAM_LIST[perm_index]) & (perm == perm_index)
        there = (line == ACROSS_LIST[perm_index]) & (perm == perm_index)
        par = par + jnp.where(here, 4.0, 0.0) - jnp.where(there, slope, 0.0)
    par_ref[p] = par

    flip_sub = jnp.where(whole, flip_z, flip_y)
    flip_lane = jnp.where(whole | outer, flip_x, flip_z)
    flip_last = jnp.where(whole, flip_y, jnp.where(outer, flip_z, flip_x))
    rows_out[p] = row_ref[flip_last]
    blocks = width // 2
    left = lax.broadcasted_iota(jnp.int32, (half, wide), 1) < width

    def gather():
        for i in range(half):
            cube[:, i * wide : (i + 1) * wide] = loose[i * step : i * step + width, :].astype(jnp.bfloat16)

    @pl.when(whole)
    def _():
        cube[...] = x_ref[0]

    @pl.when(outer)
    def _():
        for b in range(blocks):
            part = x_ref[0, :, b * wide : (b + 1) * wide].astype(jnp.float32)
            top, low = part[:half], part[half:]
            loose[pl.ds(2 * b, half, stride=step), :] = jnp.where(left, top, pltpu.roll(low, width, 1))
            loose[pl.ds(2 * b + 1, half, stride=step), :] = jnp.where(left, pltpu.roll(top, width, 1), low)
        gather()

    @pl.when(jnp.logical_not(whole | outer))
    def _():
        for b in range(blocks):
            part = x_ref[0, :, b * wide : (b + 1) * wide].astype(jnp.float32).T
            for h in range(2):
                top, low = part[h * width : h * width + half], part[h * width + half : (h + 1) * width]
                loose[pl.ds(2 * b + h, half, stride=step), :] = jnp.concatenate([top, low], 1)
        gather()

    def place(b, h):
        return jnp.where(whole, 2 * b + h, b + h * half)

    def put(b, h, value):
        held[p, pl.ds(place(b, h), width, stride=step), :] = value

    @pl.when(jnp.logical_not(swapped))
    def _():
        first, second = left_ref[flip_sub], right_ref[flip_lane]
        for base in range(0, blocks, BLOCKS):
            out = jnp.dot(first, cube[:, base * wide : (base + BLOCKS) * wide], preferred_element_type=jnp.float32)
            tall = jnp.concatenate(
                [
                    jnp.concatenate([out[:width, u * wide : (u + 1) * wide], out[width:, u * wide : (u + 1) * wide]], 1)
                    for u in range(BLOCKS)
                ],
                0,
            ).astype(jnp.bfloat16)
            done = jnp.dot(tall, second, preferred_element_type=jnp.float32)
            for u in range(BLOCKS):
                part = done[u * width : (u + 1) * width]
                put(base + u, 0, part[:, :wide])
                put(base + u, 1, part[:, wide:])

    @pl.when(swapped)
    def _():
        first, second = turn_ref[flip_lane], right_ref[flip_sub]
        for base in range(0, blocks, BLOCKS):
            stack = jnp.concatenate([cube[:, b * wide : (b + 1) * wide] for b in range(base, base + BLOCKS)], 0)
            out = lax.dot_general(first, stack, (((1,), (1,)), ((), ())), preferred_element_type=jnp.float32)
            tall = []
            for u in range(0, BLOCKS, 2):
                for h in range(2):
                    part = out[h * wide : (h + 1) * wide, u * width : (u + 2) * width]
                    tall.append(jnp.concatenate([part[:width], part[width:]], 1))
            tall = jnp.concatenate(tall, 0).astype(jnp.bfloat16)
            done = jnp.dot(tall, second, preferred_element_type=jnp.float32)
            for u in range(0, BLOCKS, 2):
                for h in range(2):
                    part = done[(u + h) * width : (u + h + 1) * width]
                    put(base + u, h, part[:, :wide])
                    put(base + u + 1, h, part[:, wide:])


def transform(particles, orientation, tilt, weight):
    count, width, area = particles.shape
    step = width + PAD
    wide = 2 * width
    consts = tables(width)
    smem = pl.BlockSpec(memory_space=pltpu.SMEM)
    vmem = pl.BlockSpec(memory_space=pltpu.VMEM)
    whole = [pl.BlockSpec(t.shape, lambda i: (0, 0, 0)) for t in consts]
    return pl.pallas_call(
        lambda *refs: transform_kernel(width, *refs),
        grid=(count,),
        in_specs=[smem, smem, smem, pl.BlockSpec((1, width, area), lambda i: (i, 0, 0))] + whole,
        out_specs=[vmem] * 4,
        out_shape=[
            pltpu.VMEM((count, width * step, wide), jnp.float32),
            pltpu.VMEM((count, width, wide), jnp.bfloat16),
            pltpu.VMEM((count, 8, wide), jnp.float32),
            pltpu.VMEM((8, 128), jnp.float32),
        ],
        scratch_shapes=[
            pltpu.VMEM((width // 2 * step, wide), jnp.float32),
            pltpu.VMEM((width, area), jnp.bfloat16),
        ],
        compiler_params=pltpu.CompilerParams(vmem_limit_bytes=32 << 20),
        name="transform",
    )(orientation, tilt, weight, particles, *consts)


def exchange_kernel(
    n_z, n_col, width, held, table, par, cls, fin, acc, slant, got1, sum1, got2, sum2, got3,
    zgot, zsum, ygot, cgot1, csum1, cgot2, csum2, cgot3, s1, r1, s2, r2, s3, r3, cs1, cr1, cs2, cr2, cs3, cr3, sz, rz, sy, ry,
):
    row, col = lax.axis_index("row"), lax.axis_index("col")
    z, x, core = row // 4, row // 2 % 2, row % 2
    band = width // n_col
    group = 2 * n_col
    member = x * n_col + col
    pair = (row + 1 - 2 * core, col)

    def mate(k):
        m = lax.rem(member + k, group)
        return m, (z * 4 + m // n_col * 2 + core, lax.rem(m, n_col))

    def far(k):
        t = lax.rem(z + k, n_z)
        return t, (t * 4 + x * 2 + core, col)

    def send(src, dst, ssem, rsem, to):
        copy = pltpu.make_async_remote_copy(
            src_ref=src, dst_ref=dst, send_sem=ssem, recv_sem=rsem, device_id=to, device_id_type=MESH
        )
        copy.start()
        return copy

    count = held.shape[0]
    wide = 2 * width
    step = width + PAD
    planes = fin.shape[0]
    inner = frequency(lax.broadcasted_iota(jnp.int32, (width, wide), 0), width).astype(jnp.float32)
    lane = lax.broadcasted_iota(jnp.int32, (width, wide), 1)
    outer = frequency(lax.rem(lane, width), width).astype(jnp.float32)
    sign = jnp.where(lane < width, 1.0, -1.0)
    for p in range(count):
        slant[p] = par[p, 1:2, :] * inner + par[p, 2:3, :] * outer

    def planes_of(t, who):
        def pair_of(i, carry):
            where, plane = i // (planes // 2), lax.rem(i, planes // 2) * 2
            start = ((t * 2 + where) * 2 + who) * planes + plane
            sums = [None, None]
            for p in range(count):
                pieces = [held[p, pl.ds(pl.multiple_of((start + u) * step, 8), width), :] for u in range(2)]
                plain = jnp.concatenate(pieces, 1)
                turned = jnp.concatenate([pltpu.roll(piece, width, 1) * sign for piece in pieces], 1)
                rhs = jnp.concatenate([plain, turned], 0).astype(jnp.bfloat16)
                value = jnp.dot(table[p], rhs, preferred_element_type=jnp.float32)
                for u in range(2):
                    limit = par[p, 0:1, :] * frequency(start + u, width).astype(jnp.float32)
                    gain = jnp.where(slant[p] + limit <= 0.0, par[p, 3:4, :], 0.0)
                    term = value[:, u * wide : (u + 1) * wide] * gain
                    sums[u] = term if p == 0 else sums[u] + term
            for u in range(2):
                acc[t, where, who, plane + u] = sums[u]
            return carry

        lax.fori_loop(0, planes, pair_of, 0, unroll=True)

    barrier = pltpu.get_barrier_semaphore()
    others = [pair] + [mate(k)[1] for k in range(1, group)] + [far(k)[1] for k in range(1, n_z)]
    for other in others:
        pl.semaphore_signal(barrier, inc=1, device_id=other, device_id_type=MESH)
    planes_of(lax.rem(z + 1, n_z), 1 - core)
    pl.semaphore_wait(barrier, len(others))

    def bands(m):
        return pl.ds(pl.multiple_of(lax.rem(m, n_col) * band, 8), band)

    small1 = send(cls, cgot1, cs1, cr1, pair)
    first = []
    for k in range(n_z):
        t = lax.rem(z + 1 + k, n_z)
        if k:
            planes_of(t, 1 - core)
        first.append(send(acc.at[t, :, 1 - core], got1.at[k], s1.at[k], r1.at[k], pair))
        planes_of(t, core)
    small1.wait()
    csum1[...] = cls[...] + cgot1[...]
    small2 = [send(csum1, cgot2.at[k], cs2.at[k], cr2.at[k], mate(k + 1)[1]) for k in range(group - 1)]
    main = planes - 1
    second, across_z = [], []
    for k in range(n_z):
        t = lax.rem(z + 1 + k, n_z)
        first[k].wait()
        for half in range(2):
            sum1[k, half] = acc[t, half, core] + got1[k, half]
        for g in range(group - 1):
            m, to = mate(g + 1)
            second.append(
                send(
                    sum1.at[k, m // n_col, pl.ds(0, main), bands(m), :], got2.at[k, g], s2.at[k, g], r2.at[k, g], to
                )
            )
        if k < n_z - 1:
            across_z.append(send(sum1.at[k, :, main], zgot.at[k], sz.at[k], rz.at[k], far(k + 1)[1]))
    for copy in small2:
        copy.wait()
    small = csum1[...]
    for k in range(group - 1):
        small = small + cgot2[k]
    csum2[...] = small
    small3 = [send(csum2, cgot3.at[k], cs3.at[k], cr3.at[k], far(k + 1)[1]) for k in range(n_z - 1)]
    third = []
    for k in range(n_z):
        for g in range(group - 1):
            second[k * (group - 1) + g].wait()
        total = sum1[k, x, pl.ds(0, main), bands(member), :]
        for g in range(group - 1):
            total = total + got2[k, g]
        sum2[k] = total
        if k < n_z - 1:
            third.append(send(sum2.at[k], got3.at[k], s3.at[k], r3.at[k], far(k + 1)[1]))
        if k == n_z // 2 - 1:
            for copy in across_z:
                copy.wait()
            for half in range(2):
                total = sum1[n_z - 1, half, main]
                for d in range(n_z - 1):
                    total = total + zgot[d, half]
                zsum[half] = total
            closing = []
            for g in range(group - 1):
                m, to = mate(g + 1)
                closing.append(send(zsum.at[m // n_col, bands(m), :], ygot.at[g], sy.at[g], ry.at[g], to))

    for copy in small3:
        copy.wait()
    small = csum2[...]
    for k in range(n_z - 1):
        small = small + cgot3[k]
    shape = (band, 2 * width)
    middle = frequency(col * band + lax.broadcasted_iota(jnp.int32, shape, 0), width)
    last = frequency(lax.broadcasted_iota(jnp.int32, shape, 1) % width, width)
    factors = []
    for plane in range(planes):
        axes = (jnp.full(shape, 1, jnp.int32) * frequency(row * planes + plane, width), middle, last)
        total = jnp.zeros(shape, jnp.float32)
        for perm in range(6):
            beam, across = 4 * axes[BEAM_LIST[perm]], axes[ACROSS_LIST[perm]]
            for tilt in range(TILTS):
                share = small[0:1, perm * TILTS + tilt : perm * TILTS + tilt + 1]
                total = total + jnp.where(beam <= (5 + 2 * tilt) * across, share, 0.0)
        factors.append(jnp.sqrt(total + wiener_offset))
    for copy in third + closing:
        copy.wait()
    for plane in range(planes):
        if plane < main:
            value = sum2[n_z - 1, plane]
            for k in range(n_z - 1):
                value = value + got3[k, plane]
        else:
            value = zsum[x, bands(member), :]
            for g in range(group - 1):
                value = value + ygot[g]
        fin[plane] = value / factors[plane]


def finish_kernel(width, fin, out):
    planes, band, _ = fin.shape
    half = band // 2
    left = lax.broadcasted_iota(jnp.int32, (half, 2 * width), 1) < width
    for plane in range(planes):
        even = fin[plane, pl.ds(0, half, stride=2), :]
        odd = fin[plane, pl.ds(1, half, stride=2), :]
        real = jnp.where(left, even, pltpu.roll(odd, width, 1))
        imag = jnp.where(left, pltpu.roll(even, width, 1), odd)
        for k in range(half):
            lanes = pl.ds(k * 2 * width, 2 * width)
            out[0, plane : plane + 1, lanes] = real[k : k + 1]
            out[1, plane : plane + 1, lanes] = imag[k : k + 1]


def finish(fin, width):
    planes, band, _ = fin.shape
    vmem = pl.BlockSpec(memory_space=pltpu.VMEM)
    return pl.pallas_call(
        lambda *refs: finish_kernel(width, *refs),
        in_specs=[vmem],
        out_specs=vmem,
        out_shape=jax.ShapeDtypeStruct((2, planes, band * width), jnp.float32),
        compiler_params=pltpu.CompilerParams(vmem_limit_bytes=32 << 20),
        name="finish",
    )(pltpu.with_memory_space_constraint(fin, pltpu.VMEM))


def exchange(held, table, par, cls, n_row, n_col, width):
    n_z = n_row // 4
    planes = width // n_row
    band = width // n_col
    group = 2 * n_col
    wide = 2 * width
    count = held.shape[0]
    operands = [pltpu.with_memory_space_constraint(a, pltpu.VMEM) for a in (held, table, par, cls)]
    vmem = pl.BlockSpec(memory_space=pltpu.VMEM)
    f32 = jnp.float32
    dma = pltpu.SemaphoreType.DMA
    return pl.pallas_call(
        lambda *refs: exchange_kernel(n_z, n_col, width, *refs),
        in_specs=[vmem] * 4,
        out_specs=vmem,
        out_shape=pltpu.VMEM((planes, band, wide), f32),
        scratch_shapes=[
            pltpu.VMEM((n_z, 2, 2, planes, width, wide), f32),
            pltpu.VMEM((count, width, wide), f32),
            pltpu.VMEM((n_z, 2, planes, width, wide), f32),
            pltpu.VMEM((n_z, 2, planes, width, wide), f32),
            pltpu.VMEM((n_z, group - 1, planes - 1, band, wide), f32),
            pltpu.VMEM((n_z, planes - 1, band, wide), f32),
            pltpu.VMEM((n_z - 1, planes - 1, band, wide), f32),
            pltpu.VMEM((n_z - 1, 2, width, wide), f32),
            pltpu.VMEM((2, width, wide), f32),
            pltpu.VMEM((group - 1, band, wide), f32),
            pltpu.VMEM((8, 128), f32),
            pltpu.VMEM((8, 128), f32),
            pltpu.VMEM((group - 1, 8, 128), f32),
            pltpu.VMEM((8, 128), f32),
            pltpu.VMEM((n_z - 1, 8, 128), f32),
            dma((n_z,)), dma((n_z,)), dma((n_z, group - 1)), dma((n_z, group - 1)),
            dma((n_z - 1,)), dma((n_z - 1,)),
            dma, dma, dma((group - 1,)), dma((group - 1,)), dma((n_z - 1,)), dma((n_z - 1,)),
            dma((n_z - 1,)), dma((n_z - 1,)), dma((group - 1,)), dma((group - 1,)),
        ],
        compiler_params=pltpu.CompilerParams(collective_id=0, has_side_effects=True, vmem_limit_bytes=32 << 20),
        name="exchange",
    )(*operands)


def solution(mesh):
    n_row, n_col = mesh.shape["row"], mesh.shape["col"]

    def body(particles, orientation, tilt, weight):
        width = particles.shape[1]
        parts = transform(particles, orientation, tilt, weight)
        return finish(exchange(*parts, n_row, n_col, width), width)

    placed = (P(("row", "col"), None, None), P(("row", "col")), P(("row", "col")), P(("row", "col")))
    return jax.shard_map(body, mesh=mesh, in_specs=placed, out_specs=P(None, "row", "col"), check_vma=False)
```

```python
import math

import jax
import jax.numpy as jnp
import numpy as np
from jax import lax
from jax.experimental import pallas as pl
from jax.experimental.pallas import tpu as pltpu
from jax.sharding import PartitionSpec as P

TILTS = 8
BEAM_LIST = (0, 0, 1, 2, 1, 2)
ACROSS_LIST = (2, 1, 2, 1, 0, 0)
wiener_offset = 1.0
MESH = pl.DeviceIdType.MESH
PAD = 8
BLOCKS = 8


def tables(width):
    index = np.arange(width)
    angle = (index[:, None] * index[None, :] % width).astype(np.float32) * np.float32(2.0 * math.pi / width)
    factor = np.float32(1.0 / math.sqrt(width))
    lefts, turns, rights, rows = [], [], [], []
    for reverse in (False, True):
        c, s = np.cos(angle) * factor, np.sin(angle) * factor
        if reverse:
            c, s = c[:, ::-1], s[:, ::-1]
        zero = np.zeros_like(c)
        lefts.append(np.concatenate([c, -s], 0))
        turns.append(np.block([[c, zero], [-s, zero], [zero, c], [zero, -s]]))
        plain, turned, blank = np.concatenate([c.T, -s.T], 1), np.concatenate([s.T, c.T], 1), np.zeros((width, 2 * width))
        rights.append(np.block([[plain, blank], [blank, plain], [turned, blank], [blank, turned]]))
        rows.append(np.concatenate([c, s], 1))
    return [jnp.asarray(np.stack(t), jnp.float32).astype(jnp.bfloat16) for t in (lefts, turns, rights, rows)]


def frequency(index, width):
    return jnp.abs(jnp.where(index < width // 2, index, index - width))


def transform_kernel(
    width, ori, tilt, weight, x_ref, left_ref, turn_ref, right_ref, row_ref, held, rows_out, par_ref, cls_ref, loose, cube
):
    p = pl.program_id(0)
    wide = 2 * width
    half = width // 2
    step = width + PAD
    orient = ori[p]
    perm = orient // 4
    flip_z = orient % 2
    flip_y = orient // 2 % 2
    parity = jnp.where((perm == 1) | (perm == 2) | (perm == 5), 1, 0)
    flip_x = (flip_z + flip_y + parity) % 2
    swapped = (perm == 1) | (perm == 4) | (perm == 5)
    whole = (perm == 0) | (perm == 5)
    outer = (perm == 2) | (perm == 4)
    scale = weight[p]

    @pl.when(p == 0)
    def _():
        cls_ref[...] = jnp.zeros_like(cls_ref)

    label = lax.broadcasted_iota(jnp.int32, cls_ref.shape, 1)
    cls_ref[...] += jnp.where(label == perm * TILTS + tilt[p], scale, 0.0)

    slope = (5 + 2 * tilt[p]).astype(jnp.float32)
    line = lax.broadcasted_iota(jnp.int32, (8, wide), 0)
    par = jnp.where(line == 3, scale, 0.0)
    for perm_index in range(6):
        here = (line == BEAM_LIST[perm_index]) & (perm == perm_index)
        there = (line == ACROSS_LIST[perm_index]) & (perm == perm_index)
        par = par + jnp.where(here, 4.0, 0.0) - jnp.where(there, slope, 0.0)
    par_ref[p] = par

    flip_sub = jnp.where(whole, flip_z, flip_y)
    flip_lane = jnp.where(whole | outer, flip_x, flip_z)
    flip_last = jnp.where(whole, flip_y, jnp.where(outer, flip_z, flip_x))
    rows_out[p] = row_ref[flip_last]
    blocks = width // 2
    left = lax.broadcasted_iota(jnp.int32, (half, wide), 1) < width

    def gather():
        for i in range(half):
            cube[:, i * wide : (i + 1) * wide] = loose[i * step : i * step + width, :].astype(jnp.bfloat16)

    @pl.when(whole)
    def _():
        cube[...] = x_ref[0]

    @pl.when(outer)
    def _():
        for b in range(blocks):
            part = x_ref[0, :, b * wide : (b + 1) * wide].astype(jnp.float32)
            top, low = part[:half], part[half:]
            loose[pl.ds(2 * b, half, stride=step), :] = jnp.where(left, top, pltpu.roll(low, width, 1))
            loose[pl.ds(2 * b + 1, half, stride=step), :] = jnp.where(left, pltpu.roll(top, width, 1), low)
        gather()

    @pl.when(jnp.logical_not(whole | outer))
    def _():
        for b in range(blocks):
            part = x_ref[0, :, b * wide : (b + 1) * wide].astype(jnp.float32).T
            for h in range(2):
                top, low = part[h * width : h * width + half], part[h * width + half : (h + 1) * width]
                loose[pl.ds(2 * b + h, half, stride=step), :] = jnp.concatenate([top, low], 1)
        gather()

    def place(b, h):
        return jnp.where(whole, 2 * b + h, b + h * half)

    def put(b, h, value):
        held[p, pl.ds(place(b, h), width, stride=step), :] = value

    @pl.when(jnp.logical_not(swapped))
    def _():
        first, second = left_ref[flip_sub], right_ref[flip_lane]
        for base in range(0, blocks, BLOCKS):
            out = jnp.dot(first, cube[:, base * wide : (base + BLOCKS) * wide], preferred_element_type=jnp.float32)
            tall = jnp.concatenate(
                [
                    jnp.concatenate([out[:width, u * wide : (u + 1) * wide], out[width:, u * wide : (u + 1) * wide]], 1)
                    for u in range(BLOCKS)
                ],
                0,
            ).astype(jnp.bfloat16)
            done = jnp.dot(tall, second, preferred_element_type=jnp.float32)
            for u in range(BLOCKS):
                part = done[u * width : (u + 1) * width]
                put(base + u, 0, part[:, :wide])
                put(base + u, 1, part[:, wide:])

    @pl.when(swapped)
    def _():
        first, second = turn_ref[flip_lane], right_ref[flip_sub]
        for base in range(0, blocks, BLOCKS):
            stack = jnp.concatenate([cube[:, b * wide : (b + 1) * wide] for b in range(base, base + BLOCKS)], 0)
            out = lax.dot_general(first, stack, (((1,), (1,)), ((), ())), preferred_element_type=jnp.float32)
            tall = []
            for u in range(0, BLOCKS, 2):
                for h in range(2):
                    part = out[h * wide : (h + 1) * wide, u * width : (u + 2) * width]
                    tall.append(jnp.concatenate([part[:width], part[width:]], 1))
            tall = jnp.concatenate(tall, 0).astype(jnp.bfloat16)
            done = jnp.dot(tall, second, preferred_element_type=jnp.float32)
            for u in range(0, BLOCKS, 2):
                for h in range(2):
                    part = done[(u + h) * width : (u + h + 1) * width]
                    put(base + u, h, part[:, :wide])
                    put(base + u + 1, h, part[:, wide:])


def transform(particles, orientation, tilt, weight):
    count, width, area = particles.shape
    step = width + PAD
    wide = 2 * width
    consts = tables(width)
    smem = pl.BlockSpec(memory_space=pltpu.SMEM)
    vmem = pl.BlockSpec(memory_space=pltpu.VMEM)
    whole = [pl.BlockSpec(t.shape, lambda i: (0, 0, 0)) for t in consts]
    return pl.pallas_call(
        lambda *refs: transform_kernel(width, *refs),
        grid=(count,),
        in_specs=[smem, smem, smem, pl.BlockSpec((1, width, area), lambda i: (i, 0, 0))] + whole,
        out_specs=[vmem] * 4,
        out_shape=[
            pltpu.VMEM((count, width * step, wide), jnp.float32),
            pltpu.VMEM((count, width, wide), jnp.bfloat16),
            pltpu.VMEM((count, 8, wide), jnp.float32),
            pltpu.VMEM((8, 128), jnp.float32),
        ],
        scratch_shapes=[
            pltpu.VMEM((width // 2 * step, wide), jnp.float32),
            pltpu.VMEM((width, area), jnp.bfloat16),
        ],
        compiler_params=pltpu.CompilerParams(vmem_limit_bytes=32 << 20),
        name="transform",
    )(*(pltpu.with_memory_space_constraint(a, pltpu.HBM) for a in (orientation, tilt, weight, particles, *consts)))


def exchange_kernel(
    n_z, n_col, width, held, table, par, cls, fin, acc, slant, got1, sum1, got2, sum2, got3,
    zgot, zsum, ygot, cgot1, csum1, cgot2, csum2, cgot3, s1, r1, s2, r2, s3, r3, cs1, cr1, cs2, cr2, cs3, cr3, sz, rz, sy, ry,
):
    row, col = lax.axis_index("row"), lax.axis_index("col")
    z, x, core = row // 4, row // 2 % 2, row % 2
    band = width // n_col
    group = 2 * n_col
    member = x * n_col + col
    pair = (row + 1 - 2 * core, col)

    def mate(k):
        m = lax.rem(member + k, group)
        return m, (z * 4 + m // n_col * 2 + core, lax.rem(m, n_col))

    def far(k):
        t = lax.rem(z + k, n_z)
        return t, (t * 4 + x * 2 + core, col)

    def send(src, dst, ssem, rsem, to):
        copy = pltpu.make_async_remote_copy(
            src_ref=src, dst_ref=dst, send_sem=ssem, recv_sem=rsem, device_id=to, device_id_type=MESH
        )
        copy.start()
        return copy

    count = held.shape[0]
    wide = 2 * width
    step = width + PAD
    planes = fin.shape[0]
    inner = frequency(lax.broadcasted_iota(jnp.int32, (width, wide), 0), width).astype(jnp.float32)
    lane = lax.broadcasted_iota(jnp.int32, (width, wide), 1)
    outer = frequency(lax.rem(lane, width), width).astype(jnp.float32)
    sign = jnp.where(lane < width, 1.0, -1.0)
    for p in range(count):
        slant[p] = par[p, 1:2, :] * inner + par[p, 2:3, :] * outer

    def planes_of(t, who):
        def pair_of(i, carry):
            where, plane = i // (planes // 2), lax.rem(i, planes // 2) * 2
            start = ((t * 2 + where) * 2 + who) * planes + plane
            sums = [None, None]
            for p in range(count):
                pieces = [held[p, pl.ds(pl.multiple_of((start + u) * step, 8), width), :] for u in range(2)]
                plain = jnp.concatenate(pieces, 1)
                turned = jnp.concatenate([pltpu.roll(piece, width, 1) * sign for piece in pieces], 1)
                rhs = jnp.concatenate([plain, turned], 0).astype(jnp.bfloat16)
                value = jnp.dot(table[p], rhs, preferred_element_type=jnp.float32)
                for u in range(2):
                    limit = par[p, 0:1, :] * frequency(start + u, width).astype(jnp.float32)
                    gain = jnp.where(slant[p] + limit <= 0.0, par[p, 3:4, :], 0.0)
                    term = value[:, u * wide : (u + 1) * wide] * gain
                    sums[u] = term if p == 0 else sums[u] + term
            for u in range(2):
                acc[t, where, who, plane + u] = sums[u]
            return carry

        lax.fori_loop(0, planes, pair_of, 0, unroll=True)

    barrier = pltpu.get_barrier_semaphore()
    others = [pair] + [mate(k)[1] for k in range(1, group)] + [far(k)[1] for k in range(1, n_z)]
    for other in others:
        pl.semaphore_signal(barrier, inc=1, device_id=other, device_id_type=MESH)
    planes_of(lax.rem(z + 1, n_z), 1 - core)
    pl.semaphore_wait(barrier, len(others))

    def bands(m):
        return pl.ds(pl.multiple_of(lax.rem(m, n_col) * band, 8), band)

    small1 = send(cls, cgot1, cs1, cr1, pair)
    first = []
    for k in range(n_z):
        t = lax.rem(z + 1 + k, n_z)
        if k:
            planes_of(t, 1 - core)
        first.append(send(acc.at[t, :, 1 - core], got1.at[k], s1.at[k], r1.at[k], pair))
        planes_of(t, core)
    small1.wait()
    csum1[...] = cls[...] + cgot1[...]
    small2 = [send(csum1, cgot2.at[k], cs2.at[k], cr2.at[k], mate(k + 1)[1]) for k in range(group - 1)]
    main = planes - 1
    second, across_z = [], []
    for k in range(n_z):
        t = lax.rem(z + 1 + k, n_z)
        first[k].wait()
        for half in range(2):
            sum1[k, half] = acc[t, half, core] + got1[k, half]
        for g in range(group - 1):
            m, to = mate(g + 1)
            second.append(
                send(
                    sum1.at[k, m // n_col, pl.ds(0, main), bands(m), :], got2.at[k, g], s2.at[k, g], r2.at[k, g], to
                )
            )
        if k < n_z - 1:
            across_z.append(send(sum1.at[k, :, main], zgot.at[k], sz.at[k], rz.at[k], far(k + 1)[1]))
    for copy in small2:
        copy.wait()
    small = csum1[...]
    for k in range(group - 1):
        small = small + cgot2[k]
    csum2[...] = small
    small3 = [send(csum2, cgot3.at[k], cs3.at[k], cr3.at[k], far(k + 1)[1]) for k in range(n_z - 1)]
    third = []
    for k in range(n_z):
        for g in range(group - 1):
            second[k * (group - 1) + g].wait()
        total = sum1[k, x, pl.ds(0, main), bands(member), :]
        for g in range(group - 1):
            total = total + got2[k, g]
        sum2[k] = total
        if k < n_z - 1:
            third.append(send(sum2.at[k], got3.at[k], s3.at[k], r3.at[k], far(k + 1)[1]))
        if k == n_z // 2 - 1:
            for copy in across_z:
                copy.wait()
            for half in range(2):
                total = sum1[n_z - 1, half, main]
                for d in range(n_z - 1):
                    total = total + zgot[d, half]
                zsum[half] = total
            closing = []
            for g in range(group - 1):
                m, to = mate(g + 1)
                closing.append(send(zsum.at[m // n_col, bands(m), :], ygot.at[g], sy.at[g], ry.at[g], to))

    for copy in small3:
        copy.wait()
    small = csum2[...]
    for k in range(n_z - 1):
        small = small + cgot3[k]
    shape = (band, 2 * width)
    middle = frequency(col * band + lax.broadcasted_iota(jnp.int32, shape, 0), width)
    last = frequency(lax.broadcasted_iota(jnp.int32, shape, 1) % width, width)
    factors = []
    for plane in range(planes):
        axes = (jnp.full(shape, 1, jnp.int32) * frequency(row * planes + plane, width), middle, last)
        total = jnp.zeros(shape, jnp.float32)
        for perm in range(6):
            beam, across = 4 * axes[BEAM_LIST[perm]], axes[ACROSS_LIST[perm]]
            for tilt in range(TILTS):
                share = small[0:1, perm * TILTS + tilt : perm * TILTS + tilt + 1]
                total = total + jnp.where(beam <= (5 + 2 * tilt) * across, share, 0.0)
        factors.append(jnp.sqrt(total + wiener_offset))
    for copy in third + closing:
        copy.wait()
    for plane in range(planes):
        if plane < main:
            value = sum2[n_z - 1, plane]
            for k in range(n_z - 1):
                value = value + got3[k, plane]
        else:
            value = zsum[x, bands(member), :]
            for g in range(group - 1):
                value = value + ygot[g]
        fin[plane] = value / factors[plane]


def finish_kernel(width, fin, out):
    planes, band, _ = fin.shape
    half = band // 2
    left = lax.broadcasted_iota(jnp.int32, (half, 2 * width), 1) < width
    for plane in range(planes):
        even = fin[plane, pl.ds(0, half, stride=2), :]
        odd = fin[plane, pl.ds(1, half, stride=2), :]
        real = jnp.where(left, even, pltpu.roll(odd, width, 1))
        imag = jnp.where(left, pltpu.roll(even, width, 1), odd)
        for k in range(half):
            lanes = pl.ds(k * 2 * width, 2 * width)
            out[0, plane : plane + 1, lanes] = real[k : k + 1]
            out[1, plane : plane + 1, lanes] = imag[k : k + 1]


def finish(fin, width):
    planes, band, _ = fin.shape
    vmem = pl.BlockSpec(memory_space=pltpu.VMEM)
    return pl.pallas_call(
        lambda *refs: finish_kernel(width, *refs),
        in_specs=[vmem],
        out_specs=vmem,
        out_shape=jax.ShapeDtypeStruct((2, planes, band * width), jnp.float32),
        compiler_params=pltpu.CompilerParams(vmem_limit_bytes=32 << 20),
        name="finish",
    )(pltpu.with_memory_space_constraint(fin, pltpu.VMEM))


def exchange(held, table, par, cls, n_row, n_col, width):
    n_z = n_row // 4
    planes = width // n_row
    band = width // n_col
    group = 2 * n_col
    wide = 2 * width
    count = held.shape[0]
    operands = [pltpu.with_memory_space_constraint(a, pltpu.VMEM) for a in (held, table, par, cls)]
    vmem = pl.BlockSpec(memory_space=pltpu.VMEM)
    f32 = jnp.float32
    dma = pltpu.SemaphoreType.DMA
    return pl.pallas_call(
        lambda *refs: exchange_kernel(n_z, n_col, width, *refs),
        in_specs=[vmem] * 4,
        out_specs=vmem,
        out_shape=pltpu.VMEM((planes, band, wide), f32),
        scratch_shapes=[
            pltpu.VMEM((n_z, 2, 2, planes, width, wide), f32),
            pltpu.VMEM((count, width, wide), f32),
            pltpu.VMEM((n_z, 2, planes, width, wide), f32),
            pltpu.VMEM((n_z, 2, planes, width, wide), f32),
            pltpu.VMEM((n_z, group - 1, planes - 1, band, wide), f32),
            pltpu.VMEM((n_z, planes - 1, band, wide), f32),
            pltpu.VMEM((n_z - 1, planes - 1, band, wide), f32),
            pltpu.VMEM((n_z - 1, 2, width, wide), f32),
            pltpu.VMEM((2, width, wide), f32),
            pltpu.VMEM((group - 1, band, wide), f32),
            pltpu.VMEM((8, 128), f32),
            pltpu.VMEM((8, 128), f32),
            pltpu.VMEM((group - 1, 8, 128), f32),
            pltpu.VMEM((8, 128), f32),
            pltpu.VMEM((n_z - 1, 8, 128), f32),
            dma((n_z,)), dma((n_z,)), dma((n_z, group - 1)), dma((n_z, group - 1)),
            dma((n_z - 1,)), dma((n_z - 1,)),
            dma, dma, dma((group - 1,)), dma((group - 1,)), dma((n_z - 1,)), dma((n_z - 1,)),
            dma((n_z - 1,)), dma((n_z - 1,)), dma((group - 1,)), dma((group - 1,)),
        ],
        compiler_params=pltpu.CompilerParams(collective_id=0, has_side_effects=True, vmem_limit_bytes=32 << 20),
        name="exchange",
    )(*operands)


def solution(mesh):
    n_row, n_col = mesh.shape["row"], mesh.shape["col"]

    def body(particles, orientation, tilt, weight):
        width = particles.shape[1]
        parts = transform(particles, orientation, tilt, weight)
        return finish(exchange(*parts, n_row, n_col, width), width)

    placed = (P(("row", "col"), None, None), P(("row", "col")), P(("row", "col")), P(("row", "col")))
    return jax.shard_map(body, mesh=mesh, in_specs=placed, out_specs=P(None, "row", "col"), check_vma=False)
```
